512 devices in a mesh: dom: 8 (over z), row: 8 (over x, y_lo), col: 8 (over y_hi, core).
Axes of the slice: x: 4, y: 8 (y_hi: 4, y_lo: 2; y = y_hi * 2 + y_lo), z: 8, core: 2. Of those that a mesh axis runs over, the one named last changes fastest.
Arguments:
- currents: bfloat16 [8, 64, 32768], P('dom', None, ('col', 'row')), may hold values from -6 to 6
- shared_basis: bfloat16 [8, 64, 32768], P('dom', None, 'col'), may hold values from -0.25 to 0.25
- self_v: bfloat16 [8, 16, 64, 64, 512], P('dom', 'row', 'col'), may hold values from -0.25 to 0.25
- self_u: bfloat16 [8, 16, 64, 64, 512], P('dom', 'row', 'col'), may hold values from -0.09375 to 0.09375
- self_rank: int32 [8, 16, 64], P('dom', 'row', 'col'), may hold values from 16 to 64
- coupling_u: bfloat16 [8, 16, 8, 16, 64, 512], P('dom', 'row', None, 'col'), may hold values from -0.0625 to 0.0625
- coupling_rank: int32 [8, 16, 8, 16], P('dom', 'row', None, 'col'), may hold values from 16 to 64
- link_tiles: int32 [8, 16, 8, 16], P('dom', 'row', None, 'col'), may hold values from 0 to 7
- incident: float32 [8, 64, 8192], P('dom', 'col', 'row'), may hold values from -6 to 6
Outputs:
- residual: float32 [8, 64, 8192], P('dom', 'col', 'row')
The draws below stay inside these ranges and needn't reach their ends.
Inputs may be any that keep to these rules, and one draw needn't show every extreme that they name: `link_tiles`: entries may repeat within a list.
All inputs are finite; a program needn't handle non-finite values.
Results may differ from the reference program's by a relative error of at most 0.0022.
Values may be sent and summed in bfloat16 or wider, within the bound.
No kernel may reach another device: no remote copies, remote signals or barrier semaphores. Data moves between devices by JAX's collectives and lax.ppermute only.
A program may use at most 64 MiB of HBM per device.

```python
import jax
import jax.numpy as jnp
from jax import lax

TILE = 512
RANK = 64
ANG = 64
LINKS = 2
PARTS_SIZE = 8
TCB = 8
ROWS = 16
COLS = 64
LINKTOT = 16


def place_ends(result, rng, least, largest):
    longest = result.shape.index(max(result.shape))
    spots = []
    for shift in (0, 1):
        where = [jax.random.randint(jax.random.fold_in(rng, axis), (), 0, length) for axis, length in enumerate(result.shape)]
        where[longest] = (where[longest] + shift) % result.shape[longest]
        spots.append(tuple(where))
    return result.at[spots[0]].set(least).at[spots[1]].set(largest)


def block_levels(key, extent, cuts, least, high):
    def one(dim, parts):
        draws = jax.random.uniform(jax.random.fold_in(jax.random.fold_in(key, 6), dim), (parts,), jnp.float32, least / len(cuts), high / len(cuts))
        return jnp.repeat(jnp.exp(draws), extent[dim] // parts).reshape((-1,) + (1,) * (len(extent) - dim - 1))

    level = one(*cuts[0])
    for cut in cuts[1:]:
        level = level * one(*cut)
    return level


def normal_values(own_key, extent, width, most, pieces=(), kind=jnp.bfloat16):
    values = jax.random.normal(own_key, extent, jnp.float32) * width
    if len(pieces) > 0:
        values = block_levels(own_key, extent, pieces, -0.22, 0.18) * values
    return jnp.clip(values, min=-most, max=most).astype(kind)


def setup_inputs(seed: int = 0) -> dict:
    seeds = jax.random.split(jax.random.key(seed), 10)
    return {
        "currents": normal_values(seeds[0], (PARTS_SIZE, ANG, COLS * TILE), 1.0, 6.0, ((0, 8), (2, 64))),
        "shared_basis": normal_values(seeds[1], (PARTS_SIZE, RANK, COLS * TILE), TILE ** -0.5, 0.25, ((0, 8), (2, 8))),
        "self_v": normal_values(seeds[2], (PARTS_SIZE, ROWS, COLS, RANK, TILE), TILE ** -0.5, 0.25, ((0, 8), (1, 8), (2, 8))),
        "self_u": normal_values(seeds[3], (PARTS_SIZE, ROWS, COLS, RANK, TILE), (COLS * RANK) ** -0.5, 0.09375, ((0, 8), (1, 8), (2, 8))),
        "self_rank": place_ends(jax.random.randint(seeds[4], (PARTS_SIZE, ROWS, COLS), RANK // 4, RANK + 1), jax.random.fold_in(seeds[4], 1), RANK // 4, RANK).astype(jnp.int32),
        "coupling_u": normal_values(seeds[5], (PARTS_SIZE, ROWS, PARTS_SIZE, LINKTOT, RANK, TILE), (PARTS_SIZE * LINKTOT * RANK) ** -0.5, 0.0625, ((0, 8), (1, 8), (3, 8))),
        "coupling_rank": place_ends(jax.random.randint(seeds[6], (PARTS_SIZE, ROWS, PARTS_SIZE, LINKTOT), RANK // 4, RANK + 1), jax.random.fold_in(seeds[6], 1), RANK // 4, RANK).astype(jnp.int32),
        "link_tiles": place_ends(jax.random.randint(seeds[7], (PARTS_SIZE, ROWS, PARTS_SIZE, LINKTOT), 0, TCB), jax.random.fold_in(seeds[7], 1), 0, TCB - 1).astype(jnp.int32),
        "incident": normal_values(seeds[8], (PARTS_SIZE, ANG, ROWS * TILE), 1.0, 6.0, ((0, 8), (1, 8), (2, 8)), jnp.float32),
    }


def reference(currents, shared_basis, self_v, self_u, self_rank, coupling_u, coupling_rank, link_tiles, incident):
    levels = jnp.arange(RANK, dtype=jnp.int32)
    current_all = currents.astype(jnp.float32).reshape(PARTS_SIZE, ANG, COLS, TILE)
    bases = shared_basis.astype(jnp.float32).reshape(PARTS_SIZE, RANK, COLS, TILE)
    basisproj = jnp.einsum("ekjn,eajn->ejka", bases, current_all).astype(jnp.bfloat16)
    flat_proj = basisproj.reshape(PARTS_SIZE * COLS, RANK, ANG)
    block_base = (jnp.arange(LINKTOT, dtype=jnp.int32) // LINKS) * TCB
    part_base = jnp.arange(PARTS_SIZE, dtype=jnp.int32)[:, None] * COLS

    def one_part(part_index):
        current_part = lax.dynamic_index_in_dim(current_all, part_index, 0, keepdims=False)
        v_part = lax.dynamic_index_in_dim(self_v, part_index, 0, keepdims=False).astype(jnp.float32)
        u_part = lax.dynamic_index_in_dim(self_u, part_index, 0, keepdims=False).astype(jnp.float32)
        rank_part = lax.dynamic_index_in_dim(self_rank, part_index, 0, keepdims=False)
        keep_self = (levels[None, None, :] < rank_part[:, :, None]).astype(jnp.float32)
        selfproj = jnp.einsum("ijkn,ajn->ijka", v_part, current_part)
        selfproj = (selfproj * keep_self[..., None]).astype(jnp.bfloat16)
        field_self = jnp.einsum("ijkn,ijka->ain", u_part, selfproj.astype(jnp.float32))
        links_part = lax.dynamic_index_in_dim(link_tiles, part_index, 0, keepdims=False)
        picks = (part_base + block_base[None, :])[None, :, :] + links_part
        chosen = jnp.take(flat_proj, picks.reshape(-1).astype(jnp.int32), axis=0)
        chosen = chosen.reshape(ROWS, PARTS_SIZE, LINKTOT, RANK, ANG)
        crank_part = lax.dynamic_index_in_dim(coupling_rank, part_index, 0, keepdims=False)
        keep_cpl = (levels < crank_part[..., None]).astype(jnp.bfloat16)
        chosen = chosen * keep_cpl[..., None]
        cu_part = lax.dynamic_index_in_dim(coupling_u, part_index, 0, keepdims=False).astype(jnp.float32)
        field_cpl = jnp.einsum("iemkn,iemka->ain", cu_part, chosen.astype(jnp.float32))
        field = (field_self + field_cpl).reshape(ANG, ROWS * TILE)
        rhs_part = lax.dynamic_index_in_dim(incident, part_index, 0, keepdims=False)
        return rhs_part - field

    return lax.map(one_part, jnp.arange(PARTS_SIZE, dtype=jnp.int32))
```

```python
import jax
import jax.numpy as jnp
from jax import lax
from jax.experimental import pallas as pl
from jax.experimental.pallas import tpu as pltpu
from jax.sharding import PartitionSpec as P

BF = jnp.bfloat16
F32 = jnp.float32
NT = (((1,), (1,)), ((), ()))


def exchange(value, axis):
    return lax.all_to_all(value, axis, split_axis=0, concat_axis=0, tiled=True)


def low_lanes(shape):
    return lax.broadcasted_iota(jnp.int32, shape, 1) < shape[1] // 2


def project_kernel(where, currents, basis, out):
    proj = lax.dot_general(currents[...], basis[...], NT, preferred_element_type=F32)
    half = proj.shape[0] // 2
    packed = jnp.concatenate([proj[:half], proj[half:]], axis=1).astype(BF)
    for peer in range(out.shape[0]):
        out[peer] = packed


def pack_kernel(arrived, currents, out):
    tile = currents.shape[1]
    half, lanes = arrived.shape[1:]
    low = low_lanes((half, lanes))
    rows = []
    for pair in range(arrived.shape[0] // 2):
        even = arrived[2 * pair].astype(F32)
        odd = arrived[2 * pair + 1].astype(F32)
        top = jnp.where(low, even, pltpu.roll(odd, lanes // 2, 1))
        bottom = jnp.where(low, pltpu.roll(even, lanes // 2, 1), odd)
        rows.append(jnp.concatenate([top, bottom], axis=0).astype(BF))
    own = currents[...]
    for peer in range(out.shape[0]):
        out[peer, :, :tile] = own
        for pair, value in enumerate(rows):
            out[peer, :, tile + pair * lanes : tile + (pair + 1) * lanes] = value


def field_kernel(self_rank, cpl_rank, links, arrived, v, u, cu, out, left, picked):
    rows, tiles, ranks, tile = v.shape
    parts, link_count = cu.shape[1:3]
    angles = arrived.shape[1]
    lanes = 2 * ranks
    low = low_lanes((angles, lanes))
    level = lax.broadcasted_iota(jnp.int32, (angles, lanes), 1)
    level = jnp.where(low, level, level - ranks)
    for pair in range(tiles // 2):
        first, second = 2 * pair, 2 * pair + 1
        both = jnp.concatenate([arrived[first, :, :tile], arrived[second, :, :tile]], axis=0)
        for t in range(rows):
            factors = v[t, first : second + 1].reshape(lanes, tile)
            product = lax.dot_general(both, factors, NT, preferred_element_type=F32)
            value = jnp.where(low, product[:angles], product[angles:])
            limit = jnp.where(low, self_rank[t, first], self_rank[t, second])
            value = jnp.where(level < limit, value, 0.0)
            left[t, :, pair * lanes : (pair + 1) * lanes] = value.astype(BF)
    for t in range(rows):
        for e in range(parts):
            at = tile + (e // 2) * lanes
            one = arrived[links[t, e, 0], :, at : at + lanes].astype(F32)
            two = arrived[links[t, e, 1], :, at : at + lanes].astype(F32)
            if e % 2 == 0:
                two = pltpu.roll(two, ranks, 1)
            else:
                one = pltpu.roll(one, ranks, 1)
            value = jnp.where(low, one, two)
            limit = jnp.where(low, cpl_rank[t, e, 0], cpl_rank[t, e, 1])
            value = jnp.where(level < limit, value, 0.0)
            picked[t, :, e * lanes : (e + 1) * lanes] = value.astype(BF)
    for t in range(rows):
        field = jnp.dot(left[t], u[t].reshape(tiles * ranks, tile), preferred_element_type=F32)
        field += jnp.dot(
            picked[t], cu[t].reshape(parts * link_count * ranks, tile), preferred_element_type=F32
        )
        out[:, t * tile : (t + 1) * tile] = field.astype(out.dtype)


def shards(
    currents, shared_basis, self_v, self_u, self_rank, coupling_u, coupling_rank, link_tiles, incident
):
    row_count = lax.axis_size("row")
    dom_count = lax.axis_size("dom")
    col_count = lax.axis_size("col")
    _, angles, tile = currents.shape
    _, window_rows, tiles, ranks, _ = self_v.shape
    link_count = link_tiles.shape[-1]
    vmem = pl.BlockSpec(memory_space=pltpu.VMEM)
    smem = pl.BlockSpec(memory_space=pltpu.SMEM)
    own = currents[0]
    where = lax.axis_index("row").astype(jnp.int32).reshape(1)
    outgoing = pl.pallas_call(
        project_kernel,
        out_shape=jax.ShapeDtypeStruct((dom_count, angles // 2, 2 * ranks), BF),
        grid_spec=pltpu.PrefetchScalarGridSpec(
            num_scalar_prefetch=1,
            grid=(1,),
            in_specs=[
                pl.BlockSpec((angles, tile), lambda i, w: (0, 0)),
                pl.BlockSpec((ranks, tile), lambda i, w: (0, w[0])),
            ],
            out_specs=pl.BlockSpec((dom_count, angles // 2, 2 * ranks), lambda i, w: (0, 0, 0)),
        ),
        name="project",
    )(where, own, shared_basis[0])
    arrived = exchange(outgoing, "dom")
    outgoing = pl.pallas_call(
        pack_kernel,
        out_shape=jax.ShapeDtypeStruct((row_count, angles, tile + dom_count * ranks), BF),
        in_specs=[vmem, vmem],
        out_specs=vmem,
        name="pack",
    )(arrived, own)
    arrived = exchange(outgoing, "row")
    partial = pl.pallas_call(
        field_kernel,
        out_shape=jax.ShapeDtypeStruct((angles, window_rows * tile), BF),
        in_specs=[smem, smem, smem, vmem, vmem, vmem, vmem],
        out_specs=vmem,
        scratch_shapes=[
            pltpu.VMEM((window_rows, angles, tiles * ranks), BF),
            pltpu.VMEM((window_rows, angles, dom_count * link_count * ranks), BF),
        ],
        name="field",
    )(self_rank[0], coupling_rank[0], link_tiles[0], arrived, self_v[0], self_u[0], coupling_u[0])
    arrived = exchange(partial.reshape(col_count, angles // col_count, window_rows * tile), "col")
    return (incident[0] - arrived.astype(F32).sum(axis=0))[None]


def solution(mesh):
    return jax.shard_map(
        shards,
        mesh=mesh,
        in_specs=(
            P("dom", None, ("col", "row")),
            P("dom", None, "col"),
            P("dom", "row", "col", None, None),
            P("dom", "row", "col", None, None),
            P("dom", "row", "col"),
            P("dom", "row", None, "col", None, None),
            P("dom", "row", None, "col"),
            P("dom", "row", None, "col"),
            P("dom", "col", "row"),
        ),
        out_specs=P("dom", "col", "row"),
        check_vma=False,
    )
```

```python
import jax
import jax.numpy as jnp
from jax import lax
from jax.experimental import pallas as pl
from jax.experimental.pallas import tpu as pltpu
from jax.sharding import PartitionSpec as P


BF = jnp.bfloat16
F32 = jnp.float32
NT = (((1,), (1,)), ((), ()))
ONCHIP = pl.BlockSpec(memory_space=pltpu.VMEM)
SCALARS = pl.BlockSpec(memory_space=pltpu.SMEM)
ANYWHERE = pl.BlockSpec(memory_space=pl.ANY)
LIMIT = pltpu.CompilerParams(vmem_limit_bytes=16 * 2**20)


def exchange(value, axis):
    return lax.all_to_all(value, axis, split_axis=0, concat_axis=0, tiled=True)


def swap(value, axis, bits):
    return lax.ppermute(value, axis, [(i, i ^ bits) for i in range(lax.axis_size(axis))])


def onchip(value):
    return pltpu.with_memory_space_constraint(value, pltpu.VMEM)


def inhbm(value):
    return pltpu.with_memory_space_constraint(value, pltpu.HBM)


def low_lanes(shape):
    return lax.broadcasted_iota(jnp.int32, shape, 1) < shape[1] // 2


def project_kernel(currents, basis, out, own, own_basis, arrivals):
    tile = currents.shape[1]
    at = pl.multiple_of(lax.axis_index("row") * tile, tile)
    copies = [
        pltpu.make_async_copy(basis.at[:, pl.ds(at, tile)], own_basis, arrivals.at[0]),
        pltpu.make_async_copy(currents, own, arrivals.at[1]),
    ]
    for copy in copies:
        copy.start()
    for copy in copies:
        copy.wait()
    proj = lax.dot_general(own[...], own_basis[...], NT, preferred_element_type=F32)
    half = proj.shape[0] // 2
    packed = jnp.concatenate([proj[:half], proj[half:]], axis=1).astype(BF)
    for peer in range(out.shape[0]):
        out[peer] = packed


def limits_kernel(self_rank, cpl_rank, out):
    rows, pairs = self_rank.shape[0], self_rank.shape[1] // 2
    low = low_lanes((1, out.shape[-1]))
    for t in range(rows):
        for q in range(pairs):
            out[t, q : q + 1] = jnp.where(low, self_rank[t, 2 * q], self_rank[t, 2 * q + 1])
        for e in range(cpl_rank.shape[1]):
            at = pairs + e
            out[t, at : at + 1] = jnp.where(low, cpl_rank[t, e, 0], cpl_rank[t, e, 1])


def pair_of(slot):
    return slot ^ (lax.axis_index("row") // 2)


def projected(currents, factors, limits):
    odd = lax.axis_index("row") % 2
    angles = currents.shape[1]
    lanes = limits.shape[-1]
    both = jnp.concatenate([currents[odd], currents[1 - odd]], axis=0)
    product = lax.dot_general(
        both, factors.reshape(lanes, factors.shape[-1]), NT, preferred_element_type=F32
    )
    value = jnp.where(low_lanes((angles, lanes)), product[:angles], product[angles:])
    return jnp.where(levels((angles, lanes)) < limits, value, 0.0).astype(BF)


def levels(shape):
    level = lax.broadcasted_iota(jnp.int32, shape, 1)
    return jnp.where(low_lanes(shape), level, level - shape[1] // 2)


def self_kernel(limits, near, far2, far6, v_hbm, u_hbm, out, v, u, arrivals):
    rows, _, ranks, tile = v.shape
    fetch = [
        pltpu.make_async_copy(src, dst, arrivals.at[i])
        for i, (src, dst) in enumerate(((v_hbm, v), (u_hbm, u)))
    ]
    for copy in fetch:
        copy.start()
    fetch[0].wait()
    slots = ((0, near), (1, far2), (3, far6))
    left = []
    for t in range(rows):
        for slot, currents in slots:
            pair = pair_of(slot)
            left.append(
                projected(currents, v[t, pl.ds(2 * pair, 2)], limits[t, pl.ds(pair, 1)])
            )
    fetch[1].wait()
    for t in range(rows):
        total = None
        for i, (slot, _) in enumerate(slots):
            factors = u[t, pl.ds(2 * pair_of(slot), 2)].reshape(2 * ranks, tile)
            part = jnp.dot(left[t * len(slots) + i], factors, preferred_element_type=F32)
            total = part if total is None else total + part
        out[:, t * tile : (t + 1) * tile] = total


def coupled_kernel(
    links, limits, arrived, far4, field, cu, v_hbm, u_hbm, out, picked, last_v, last_u, arrivals
):
    rows, parts, link_count, ranks, tile = cu.shape
    angles = field.shape[0]
    half, lanes = arrived.shape[1:]
    block_tiles = arrived.shape[0] // parts
    pairs = limits.shape[1] - parts
    low = low_lanes((half, lanes))
    level = levels((angles, lanes))
    last = pl.ds(2 * pair_of(2), 2)
    fetch = [
        pltpu.make_async_copy(src.at[:, last], dst, arrivals.at[i])
        for i, (src, dst) in enumerate(((v_hbm, last_v), (u_hbm, last_u)))
    ]
    for copy in fetch:
        copy.start()
    for t in range(rows):
        for e in range(parts):
            one = arrived[e * block_tiles + links[t, e, 0]].astype(F32)
            two = arrived[e * block_tiles + links[t, e, 1]].astype(F32)
            top = jnp.where(low, one, pltpu.roll(two, ranks, 1))
            bottom = jnp.where(low, pltpu.roll(one, ranks, 1), two)
            value = jnp.concatenate([top, bottom], axis=0)
            value = jnp.where(level < limits[t, pairs + e : pairs + e + 1], value, 0.0)
            picked[t, :, e * lanes : (e + 1) * lanes] = value.astype(BF)
    totals = []
    for t in range(rows):
        total = field[:, t * tile : (t + 1) * tile]
        total += jnp.dot(
            picked[t], cu[t].reshape(parts * link_count * ranks, tile), preferred_element_type=F32
        )
        totals.append(total)
    for copy in fetch:
        copy.wait()
    for t in range(rows):
        left = projected(far4, last_v[t], limits[t, pl.ds(pair_of(2), 1)])
        total = totals[t] + jnp.dot(
            left, last_u[t].reshape(lanes, tile), preferred_element_type=F32
        )
        out[:, t * tile : (t + 1) * tile] = total.astype(out.dtype)


def residual(
    currents, shared_basis, self_v, self_u, self_rank, coupling_u, coupling_rank, link_tiles, incident
):
    row_count = lax.axis_size("row")
    dom_count = lax.axis_size("dom")
    col_count = lax.axis_size("col")
    _, angles, tile = currents.shape
    _, window_rows, tiles, ranks, _ = self_v.shape
    link_count = link_tiles.shape[-1]
    own = currents[0]
    neighbour = swap(own, "row", 1)
    outgoing = pl.pallas_call(
        project_kernel,
        out_shape=pltpu.VMEM((dom_count * row_count, angles // 2, 2 * ranks), BF),
        in_specs=[ANYWHERE, ANYWHERE],
        out_specs=ONCHIP,
        scratch_shapes=[
            pltpu.VMEM((angles, tile), BF),
            pltpu.VMEM((ranks, tile), BF),
            pltpu.SemaphoreType.DMA((2,)),
        ],
        compiler_params=LIMIT,
        name="project",
    )(inhbm(own), inhbm(shared_basis[0]))
    arrived = exchange(outgoing, ("dom", "row"))
    near = jnp.stack([own, neighbour])
    far = {}
    for bits in (2, 6, 4):
        far[bits] = swap(near, "row", bits)
    limits = pl.pallas_call(
        limits_kernel,
        out_shape=pltpu.VMEM((window_rows, tiles // 2 + dom_count, 2 * ranks), jnp.int32),
        in_specs=[SCALARS, SCALARS],
        out_specs=ONCHIP,
        compiler_params=LIMIT,
        name="limits",
    )(self_rank[0], coupling_rank[0])
    field = pl.pallas_call(
        self_kernel,
        out_shape=pltpu.VMEM((angles, window_rows * tile), F32),
        in_specs=[ONCHIP] * 4 + [ANYWHERE] * 2,
        out_specs=ONCHIP,
        scratch_shapes=[
            pltpu.VMEM(self_v.shape[1:], BF),
            pltpu.VMEM(self_u.shape[1:], BF),
            pltpu.SemaphoreType.DMA((2,)),
        ],
        compiler_params=LIMIT,
        name="selfpart",
    )(*map(onchip, (limits, near, far[2], far[6])), inhbm(self_v[0]), inhbm(self_u[0]))
    partial = pl.pallas_call(
        coupled_kernel,
        out_shape=pltpu.VMEM((angles, window_rows * tile), BF),
        in_specs=[SCALARS] + [ONCHIP] * 5 + [ANYWHERE] * 2,
        out_specs=ONCHIP,
        scratch_shapes=[
            pltpu.VMEM((window_rows, angles, dom_count * link_count * ranks), BF),
            pltpu.VMEM((window_rows, 2, ranks, tile), BF),
            pltpu.VMEM((window_rows, 2, ranks, tile), BF),
            pltpu.SemaphoreType.DMA((2,)),
        ],
        compiler_params=LIMIT,
        name="coupled",
    )(
        link_tiles[0],
        *map(onchip, (limits, arrived, far[4], field, coupling_u[0])),
        inhbm(self_v[0]),
        inhbm(self_u[0]),
    )
    arrived = exchange(partial.reshape(col_count, angles // col_count, window_rows * tile), "col")
    return (incident[0] - arrived.astype(F32).sum(axis=0))[None]


def solution(mesh):
    return jax.shard_map(
        residual,
        mesh=mesh,
        in_specs=(
            P("dom", None, ("col", "row")),
            P("dom", None, "col"),
            P("dom", "row", "col", None, None),
            P("dom", "row", "col", None, None),
            P("dom", "row", "col"),
            P("dom", "row", None, "col", None, None),
            P("dom", "row", None, "col"),
            P("dom", "row", None, "col"),
            P("dom", "col", "row"),
        ),
        out_specs=P("dom", "col", "row"),
        check_vma=False,
    )
```

```python
import jax
import jax.numpy as jnp
from jax import lax
from jax.experimental import pallas as pl
from jax.experimental.pallas import tpu as pltpu
from jax.sharding import PartitionSpec as P


BF = jnp.bfloat16
F32 = jnp.float32
NT = (((1,), (1,)), ((), ()))
ONCHIP = pl.BlockSpec(memory_space=pltpu.VMEM)
SCALARS = pl.BlockSpec(memory_space=pltpu.SMEM)
ANYWHERE = pl.BlockSpec(memory_space=pl.ANY)
LIMIT = pltpu.CompilerParams(vmem_limit_bytes=16 * 2**20)


def exchange(value, axis):
    return lax.all_to_all(value, axis, split_axis=0, concat_axis=0, tiled=True)


def swap(value, axis, bits):
    return lax.ppermute(value, axis, [(i, i ^ bits) for i in range(lax.axis_size(axis))])


def onchip(value):
    return pltpu.with_memory_space_constraint(value, pltpu.VMEM)


def inhbm(value):
    return pltpu.with_memory_space_constraint(value, pltpu.HBM)


def low_lanes(shape):
    return lax.broadcasted_iota(jnp.int32, shape, 1) < shape[1] // 2


def project_kernel(currents, basis, out, own, own_basis, arrivals):
    tile = currents.shape[1]
    at = pl.multiple_of(lax.axis_index("row") * tile, tile)
    copies = [
        pltpu.make_async_copy(basis.at[:, pl.ds(at, tile)], own_basis, arrivals.at[0]),
        pltpu.make_async_copy(currents, own, arrivals.at[1]),
    ]
    for copy in copies:
        copy.start()
    for copy in copies:
        copy.wait()
    proj = lax.dot_general(own[...], own_basis[...], NT, preferred_element_type=F32)
    half = proj.shape[0] // 2
    packed = jnp.concatenate([proj[:half], proj[half:]], axis=1).astype(BF)
    for peer in range(out.shape[0]):
        out[peer] = packed


def limits_kernel(self_rank, cpl_rank, out):
    rows, pairs = self_rank.shape[0], self_rank.shape[1] // 2
    low = low_lanes((1, out.shape[-1]))
    for t in range(rows):
        for q in range(pairs):
            out[t, q : q + 1] = jnp.where(low, self_rank[t, 2 * q], self_rank[t, 2 * q + 1])
        for e in range(cpl_rank.shape[1]):
            at = pairs + e
            out[t, at : at + 1] = jnp.where(low, cpl_rank[t, e, 0], cpl_rank[t, e, 1])


def pair_of(slot):
    return slot ^ (lax.axis_index("row") // 2)


def projected(currents, factors, limits):
    odd = lax.axis_index("row") % 2
    angles = currents.shape[1]
    lanes = limits.shape[-1]
    both = jnp.concatenate([currents[odd], currents[1 - odd]], axis=0)
    product = lax.dot_general(
        both, factors.reshape(lanes, factors.shape[-1]), NT, preferred_element_type=F32
    )
    value = jnp.where(low_lanes((angles, lanes)), product[:angles], product[angles:])
    return jnp.where(levels((angles, lanes)) < limits, value, 0.0).astype(BF)


def levels(shape):
    level = lax.broadcasted_iota(jnp.int32, shape, 1)
    return jnp.where(low_lanes(shape), level, level - shape[1] // 2)


def self_kernel(slots, limits, currents, v_hbm, u_hbm, out, v, u, arrivals, before=None):
    rows, ranks, tile = v.shape[1], v.shape[3], v.shape[4]
    fetch = []
    for src, dst in ((v_hbm, v), (u_hbm, u)):
        for i, slot in enumerate(slots):
            pair = pl.ds(2 * pair_of(slot), 2)
            fetch.append(
                pltpu.make_async_copy(src.at[:, pair], dst.at[i], arrivals.at[len(fetch)])
            )
    for copy in fetch:
        copy.start()
    left = {}
    for i, slot in enumerate(slots):
        fetch[i].wait()
        for t in range(rows):
            left[t, i] = projected(currents[i], v[i, t], limits[t, pl.ds(pair_of(slot), 1)])
    for copy in fetch[len(slots) :]:
        copy.wait()
    for t in range(rows):
        at = slice(t * tile, (t + 1) * tile)
        weights = jnp.concatenate([left[t, i] for i in range(len(slots))], axis=1)
        factors = jnp.concatenate([u[i, t].reshape(2 * ranks, tile) for i in range(len(slots))], axis=0)
        total = jnp.dot(weights, factors, preferred_element_type=F32)
        out[:, at] = total if before is None else before[:, at] + total


def self_first_kernel(limits, near, far4, v_hbm, u_hbm, out, v, u, arrivals):
    self_kernel((0, 2), limits, (near, far4), v_hbm, u_hbm, out, v, u, arrivals)


def self_second_kernel(limits, far2, far6, before, v_hbm, u_hbm, out, v, u, arrivals):
    self_kernel((1, 3), limits, (far2, far6), v_hbm, u_hbm, out, v, u, arrivals, before)


def coupled_kernel(links, limits, arrived, field, cu, out, picked):
    rows, parts, link_count, ranks, tile = cu.shape
    angles = field.shape[0]
    half, lanes = arrived.shape[1:]
    block_tiles = arrived.shape[0] // parts
    pairs = limits.shape[1] - parts
    low = low_lanes((half, lanes))
    level = levels((angles, lanes))
    for t in range(rows):
        for e in range(parts):
            one = arrived[e * block_tiles + links[t, e, 0]].astype(F32)
            two = arrived[e * block_tiles + links[t, e, 1]].astype(F32)
            top = jnp.where(low, one, pltpu.roll(two, ranks, 1))
            bottom = jnp.where(low, pltpu.roll(one, ranks, 1), two)
            value = jnp.concatenate([top, bottom], axis=0)
            value = jnp.where(level < limits[t, pairs + e : pairs + e + 1], value, 0.0)
            picked[t, :, e * lanes : (e + 1) * lanes] = value.astype(BF)
    for t in range(rows):
        total = field[:, t * tile : (t + 1) * tile] + jnp.dot(
            picked[t], cu[t].reshape(parts * link_count * ranks, tile), preferred_element_type=F32
        )
        out[:, t * tile : (t + 1) * tile] = total.astype(out.dtype)


def residual(
    currents, shared_basis, self_v, self_u, self_rank, coupling_u, coupling_rank, link_tiles, incident
):
    row_count = lax.axis_size("row")
    dom_count = lax.axis_size("dom")
    col_count = lax.axis_size("col")
    _, angles, tile = currents.shape
    _, window_rows, tiles, ranks, _ = self_v.shape
    link_count = link_tiles.shape[-1]
    own = currents[0]
    neighbour = swap(own, "row", 1)
    outgoing = pl.pallas_call(
        project_kernel,
        out_shape=pltpu.VMEM((dom_count * row_count, angles // 2, 2 * ranks), BF),
        in_specs=[ANYWHERE, ANYWHERE],
        out_specs=ONCHIP,
        scratch_shapes=[
            pltpu.VMEM((angles, tile), BF),
            pltpu.VMEM((ranks, tile), BF),
            pltpu.SemaphoreType.DMA((2,)),
        ],
        compiler_params=LIMIT,
        name="project",
    )(inhbm(own), inhbm(shared_basis[0]))
    arrived = exchange(outgoing, ("dom", "row"))
    near = jnp.stack([own, neighbour])
    far = {}
    for bits in (4, 2, 6):
        far[bits] = swap(near, "row", bits)
    limits = pl.pallas_call(
        limits_kernel,
        out_shape=pltpu.VMEM((window_rows, tiles // 2 + dom_count, 2 * ranks), jnp.int32),
        in_specs=[SCALARS, SCALARS],
        out_specs=ONCHIP,
        compiler_params=LIMIT,
        name="limits",
    )(self_rank[0], coupling_rank[0])
    field = ()
    for kernel, currents_in in (
        (self_first_kernel, (near, far[4])), (self_second_kernel, (far[2], far[6]))
    ):
        onchip_in = (limits, *currents_in, *field)
        pair_block = (2, window_rows, 2, ranks, tile)
        field = (
            pl.pallas_call(
                kernel,
                out_shape=pltpu.VMEM((angles, window_rows * tile), F32),
                in_specs=[ONCHIP] * len(onchip_in) + [ANYWHERE] * 2,
                out_specs=ONCHIP,
                scratch_shapes=[
                    pltpu.VMEM(pair_block, BF),
                    pltpu.VMEM(pair_block, BF),
                    pltpu.SemaphoreType.DMA((4,)),
                ],
                compiler_params=LIMIT,
            )(*map(onchip, onchip_in), inhbm(self_v[0]), inhbm(self_u[0])),
        )
    partial = pl.pallas_call(
        coupled_kernel,
        out_shape=pltpu.VMEM((angles, window_rows * tile), BF),
        in_specs=[SCALARS] + [ONCHIP] * 4,
        out_specs=ONCHIP,
        scratch_shapes=[pltpu.VMEM((window_rows, angles, dom_count * link_count * ranks), BF)],
        compiler_params=LIMIT,
        name="coupled",
    )(link_tiles[0], *map(onchip, (limits, arrived, *field, coupling_u[0])))
    arrived = exchange(partial.reshape(col_count, angles // col_count, window_rows * tile), "col")
    return (incident[0] - arrived.astype(F32).sum(axis=0))[None]


def solution(mesh):
    return jax.shard_map(
        residual,
        mesh=mesh,
        in_specs=(
            P("dom", None, ("col", "row")),
            P("dom", None, "col"),
            P("dom", "row", "col", None, None),
            P("dom", "row", "col", None, None),
            P("dom", "row", "col"),
            P("dom", "row", None, "col", None, None),
            P("dom", "row", None, "col"),
            P("dom", "row", None, "col"),
            P("dom", "col", "row"),
        ),
        out_specs=P("dom", "col", "row"),
        check_vma=False,
    )
```

```python
import jax
import jax.numpy as jnp
from jax import lax
from jax.experimental import pallas as pl
from jax.experimental.pallas import tpu as pltpu
from jax.sharding import PartitionSpec as P


BF = jnp.bfloat16
F32 = jnp.float32
NT = (((1,), (1,)), ((), ()))
ONCHIP = pl.BlockSpec(memory_space=pltpu.VMEM)
ANYWHERE = pl.BlockSpec(memory_space=pl.ANY)
LIMIT = pltpu.CompilerParams(vmem_limit_bytes=16 * 2**20)


def exchange(value, axis):
    return lax.all_to_all(value, axis, split_axis=0, concat_axis=0, tiled=True)


def swap(value, axis, bits):
    return lax.ppermute(value, axis, [(i, i ^ bits) for i in range(lax.axis_size(axis))])


def onchip(value):
    return pltpu.with_memory_space_constraint(value, pltpu.VMEM)


def inhbm(value):
    return pltpu.with_memory_space_constraint(value, pltpu.HBM)


def low_lanes(shape):
    return lax.broadcasted_iota(jnp.int32, shape, 1) < shape[1] // 2


def project_kernel(currents, basis, out, own, own_basis, arrivals):
    tile = currents.shape[1]
    at = pl.multiple_of(lax.axis_index("row") * tile, tile)
    copies = [
        pltpu.make_async_copy(basis.at[:, pl.ds(at, tile)], own_basis, arrivals.at[0]),
        pltpu.make_async_copy(currents, own, arrivals.at[1]),
    ]
    for copy in copies:
        copy.start()
    for copy in copies:
        copy.wait()
    proj = lax.dot_general(own[...], own_basis[...], NT, preferred_element_type=F32)
    half = proj.shape[0] // 2
    packed = jnp.concatenate([proj[:half], proj[half:]], axis=1).astype(BF)
    for peer in range(out.shape[0]):
        out[peer] = packed


def limits_kernel(self_rank, cpl_rank, out):
    rows, pairs = self_rank.shape[0], self_rank.shape[1] // 2
    low = low_lanes((1, out.shape[-1]))
    for t in range(rows):
        own = self_rank[t : t + 1, :]
        for q in range(pairs):
            out[t, q : q + 1] = jnp.where(low, own[0, 2 * q], own[0, 2 * q + 1])
        for e in range(cpl_rank.shape[1]):
            pair = cpl_rank[t, e : e + 1, :]
            out[t, pairs + e : pairs + e + 1] = jnp.where(low, pair[0, 0], pair[0, 1])


def pair_of(slot):
    return slot ^ (lax.axis_index("row") // 2)


def projected(currents, factors, limits):
    odd = lax.axis_index("row") % 2
    angles = currents.shape[1]
    lanes = limits.shape[-1]
    both = jnp.concatenate([currents[odd], currents[1 - odd]], axis=0)
    product = lax.dot_general(
        both, factors.reshape(lanes, factors.shape[-1]), NT, preferred_element_type=F32
    )
    value = jnp.where(low_lanes((angles, lanes)), product[:angles], product[angles:])
    return jnp.where(levels((angles, lanes)) < limits, value, 0.0).astype(BF)


def levels(shape):
    level = lax.broadcasted_iota(jnp.int32, shape, 1)
    return jnp.where(low_lanes(shape), level, level - shape[1] // 2)


def self_kernel(slots, limits, currents, v_hbm, u_hbm, out, v, u, arrivals, before=None):
    rows, ranks, tile = v.shape[1], v.shape[3], v.shape[4]
    fetch = []
    for src, dst in ((v_hbm, v), (u_hbm, u)):
        for i, slot in enumerate(slots):
            pair = pl.ds(2 * pair_of(slot), 2)
            fetch.append(
                pltpu.make_async_copy(src.at[:, pair], dst.at[i], arrivals.at[len(fetch)])
            )
    for copy in fetch:
        copy.start()
    left = {}
    for i, slot in enumerate(slots):
        fetch[i].wait()
        for t in range(rows):
            left[t, i] = projected(currents[i], v[i, t], limits[t, pl.ds(pair_of(slot), 1)])
    for copy in fetch[len(slots) :]:
        copy.wait()
    for t in range(rows):
        at = slice(t * tile, (t + 1) * tile)
        weights = jnp.concatenate([left[t, i] for i in range(len(slots))], axis=1)
        factors = jnp.concatenate([u[i, t].reshape(2 * ranks, tile) for i in range(len(slots))], axis=0)
        total = jnp.dot(weights, factors, preferred_element_type=F32)
        out[:, at] = total if before is None else before[:, at] + total


def self_first_kernel(limits, near, far4, v_hbm, u_hbm, out, v, u, arrivals):
    self_kernel((0, 2), limits, (near, far4), v_hbm, u_hbm, out, v, u, arrivals)


def self_second_kernel(limits, far2, far6, before, v_hbm, u_hbm, out, v, u, arrivals):
    self_kernel((1, 3), limits, (far2, far6), v_hbm, u_hbm, out, v, u, arrivals, before)


def coupled_kernel(links, limits, arrived, field, cu, out, picked):
    rows, parts, link_count, ranks, tile = cu.shape
    angles = field.shape[0]
    half, lanes = arrived.shape[1:]
    block_tiles = arrived.shape[0] // parts
    pairs = limits.shape[1] - parts
    low = low_lanes((half, lanes))
    level = levels((angles, lanes))
    for t in range(rows):
        for e in range(parts):
            link = links[t, e : e + 1, :]
            one = arrived[e * block_tiles + link[0, 0]].astype(F32)
            two = arrived[e * block_tiles + link[0, 1]].astype(F32)
            top = jnp.where(low, one, pltpu.roll(two, ranks, 1))
            bottom = jnp.where(low, pltpu.roll(one, ranks, 1), two)
            value = jnp.concatenate([top, bottom], axis=0)
            value = jnp.where(level < limits[t, pairs + e : pairs + e + 1], value, 0.0)
            picked[t, :, e * lanes : (e + 1) * lanes] = value.astype(BF)
    for t in range(rows):
        total = field[:, t * tile : (t + 1) * tile] + jnp.dot(
            picked[t], cu[t].reshape(parts * link_count * ranks, tile), preferred_element_type=F32
        )
        out[:, t * tile : (t + 1) * tile] = total.astype(out.dtype)


def residual(
    currents, shared_basis, self_v, self_u, self_rank, coupling_u, coupling_rank, link_tiles, incident
):
    row_count = lax.axis_size("row")
    dom_count = lax.axis_size("dom")
    col_count = lax.axis_size("col")
    _, angles, tile = currents.shape
    _, window_rows, tiles, ranks, _ = self_v.shape
    link_count = link_tiles.shape[-1]
    own = currents[0]
    neighbour = swap(own, "row", 1)
    outgoing = pl.pallas_call(
        project_kernel,
        out_shape=pltpu.VMEM((dom_count * row_count, angles // 2, 2 * ranks), BF),
        in_specs=[ANYWHERE, ANYWHERE],
        out_specs=ONCHIP,
        scratch_shapes=[
            pltpu.VMEM((angles, tile), BF),
            pltpu.VMEM((ranks, tile), BF),
            pltpu.SemaphoreType.DMA((2,)),
        ],
        compiler_params=LIMIT,
        name="project",
    )(inhbm(own), inhbm(shared_basis[0]))
    arrived = exchange(outgoing, ("dom", "row"))
    near = jnp.stack([own, neighbour])
    far = {}
    for bits in (4, 6, 2):
        far[bits] = swap(near, "row", bits)
    limits = pl.pallas_call(
        limits_kernel,
        out_shape=pltpu.VMEM((window_rows, tiles // 2 + dom_count, 2 * ranks), jnp.int32),
        in_specs=[ONCHIP, ONCHIP],
        out_specs=ONCHIP,
        compiler_params=LIMIT,
        name="limits",
    )(onchip(self_rank[0]), onchip(coupling_rank[0]))
    field = ()
    for kernel, currents_in in (
        (self_first_kernel, (near, far[4])), (self_second_kernel, (far[2], far[6]))
    ):
        onchip_in = (limits, *currents_in, *field)
        pair_block = (2, window_rows, 2, ranks, tile)
        field = (
            pl.pallas_call(
                kernel,
                out_shape=pltpu.VMEM((angles, window_rows * tile), F32),
                in_specs=[ONCHIP] * len(onchip_in) + [ANYWHERE] * 2,
                out_specs=ONCHIP,
                scratch_shapes=[
                    pltpu.VMEM(pair_block, BF),
                    pltpu.VMEM(pair_block, BF),
                    pltpu.SemaphoreType.DMA((4,)),
                ],
                compiler_params=LIMIT,
            )(*map(onchip, onchip_in), inhbm(self_v[0]), inhbm(self_u[0])),
        )
    partial = pl.pallas_call(
        coupled_kernel,
        out_shape=pltpu.VMEM((angles, window_rows * tile), BF),
        in_specs=[ONCHIP] * 5,
        out_specs=ONCHIP,
        scratch_shapes=[pltpu.VMEM((window_rows, angles, dom_count * link_count * ranks), BF)],
        compiler_params=LIMIT,
        name="coupled",
    )(*map(onchip, (link_tiles[0], limits, arrived, *field, coupling_u[0])))
    arrived = exchange(partial.reshape(col_count, angles // col_count, window_rows * tile), "col")
    return (incident[0] - arrived.astype(F32).sum(axis=0))[None]


def solution(mesh):
    return jax.shard_map(
        residual,
        mesh=mesh,
        in_specs=(
            P("dom", None, ("col", "row")),
            P("dom", None, "col"),
            P("dom", "row", "col", None, None),
            P("dom", "row", "col", None, None),
            P("dom", "row", "col"),
            P("dom", "row", None, "col", None, None),
            P("dom", "row", None, "col"),
            P("dom", "row", None, "col"),
            P("dom", "col", "row"),
        ),
        out_specs=P("dom", "col", "row"),
        check_vma=False,
    )
```

```python
import jax
import jax.numpy as jnp
from jax import lax
from jax.experimental import pallas as pl
from jax.experimental.pallas import tpu as pltpu
from jax.sharding import PartitionSpec as P


BF = jnp.bfloat16
F32 = jnp.float32
NT = (((1,), (1,)), ((), ()))
ONCHIP = pl.BlockSpec(memory_space=pltpu.VMEM)
ANYWHERE = pl.BlockSpec(memory_space=pl.ANY)
LIMIT = pltpu.CompilerParams(vmem_limit_bytes=16 * 2**20)


def exchange(value, axis):
    return lax.all_to_all(value, axis, split_axis=0, concat_axis=0, tiled=True)


def swap(value, axis, bits):
    return lax.ppermute(value, axis, [(i, i ^ bits) for i in range(lax.axis_size(axis))])


def onchip(value):
    return pltpu.with_memory_space_constraint(value, pltpu.VMEM)


def inhbm(value):
    return pltpu.with_memory_space_constraint(value, pltpu.HBM)


def low_lanes(shape):
    return lax.broadcasted_iota(jnp.int32, shape, 1) < shape[1] // 2


def project_kernel(currents, basis, out):
    tile = currents.shape[1]
    own_basis = basis[:, pl.ds(pl.multiple_of(lax.axis_index("row") * tile, tile), tile)]
    proj = lax.dot_general(currents[...], own_basis, NT, preferred_element_type=F32)
    half = proj.shape[0] // 2
    packed = jnp.concatenate([proj[:half], proj[half:]], axis=1).astype(BF)
    for peer in range(out.shape[0]):
        out[peer] = packed


def lanes_kernel(out):
    out[...] = lax.broadcasted_iota(jnp.int32, out.shape, 1)


def limits_kernel(self_rank, cpl_rank, lane, out):
    rows, pairs = self_rank.shape[0], self_rank.shape[1] // 2
    low = lane[:1] < out.shape[-1] // 2
    for t in range(rows):
        own = self_rank[t : t + 1, :]
        for q in range(pairs):
            out[t, q : q + 1] = jnp.where(low, own[0, 2 * q], own[0, 2 * q + 1])
        for e in range(cpl_rank.shape[1]):
            pair = cpl_rank[t, e : e + 1, :]
            out[t, pairs + e : pairs + e + 1] = jnp.where(low, pair[0, 0], pair[0, 1])


def pair_of(slot):
    return slot ^ (lax.axis_index("row") // 2)


def projected(currents, factors, limits):
    odd = lax.axis_index("row") % 2
    angles = currents.shape[1]
    lanes = limits.shape[-1]
    both = jnp.concatenate([currents[odd], currents[1 - odd]], axis=0)
    product = lax.dot_general(
        both, factors.reshape(lanes, factors.shape[-1]), NT, preferred_element_type=F32
    )
    value = jnp.where(low_lanes((angles, lanes)), product[:angles], product[angles:])
    return jnp.where(levels((angles, lanes)) < limits, value, 0.0).astype(BF)


def levels(shape):
    level = lax.broadcasted_iota(jnp.int32, shape, 1)
    return jnp.where(low_lanes(shape), level, level - shape[1] // 2)


def self_kernel(slots, limits, currents, v_hbm, u_hbm, out, v, u, arrivals, before=None):
    rows, ranks, tile = v.shape[1], v.shape[3], v.shape[4]
    fetch = []
    for src, dst in ((v_hbm, v), (u_hbm, u)):
        for i, slot in enumerate(slots):
            pair = pl.ds(2 * pair_of(slot), 2)
            fetch.append(
                pltpu.make_async_copy(src.at[:, pair], dst.at[i], arrivals.at[len(fetch)])
            )
    for copy in fetch:
        copy.start()
    left = {}
    for i, slot in enumerate(slots):
        fetch[i].wait()
        for t in range(rows):
            left[t, i] = projected(currents[i], v[i, t], limits[t, pl.ds(pair_of(slot), 1)])
    for copy in fetch[len(slots) :]:
        copy.wait()
    for t in range(rows):
        at = slice(t * tile, (t + 1) * tile)
        weights = jnp.concatenate([left[t, i] for i in range(len(slots))], axis=1)
        factors = jnp.concatenate([u[i, t].reshape(2 * ranks, tile) for i in range(len(slots))], axis=0)
        total = jnp.dot(weights, factors, preferred_element_type=F32)
        out[:, at] = total if before is None else before[:, at] + total


def self_first_kernel(limits, near, far4, v_hbm, u_hbm, out, v, u, arrivals):
    self_kernel((0, 2), limits, (near, far4), v_hbm, u_hbm, out, v, u, arrivals)


def self_second_kernel(limits, far2, far6, before, v_hbm, u_hbm, out, v, u, arrivals):
    self_kernel((1, 3), limits, (far2, far6), v_hbm, u_hbm, out, v, u, arrivals, before)


def coupled_kernel(links, limits, arrived, field, cu, out, picked):
    rows, parts, link_count, ranks, tile = cu.shape
    angles = field.shape[0]
    half, lanes = arrived.shape[1:]
    block_tiles = arrived.shape[0] // parts
    pairs = limits.shape[1] - parts
    low = low_lanes((half, lanes))
    level = levels((angles, lanes))
    for t in range(rows):
        for e in range(parts):
            link = links[t, e : e + 1, :]
            one = arrived[e * block_tiles + link[0, 0]].astype(F32)
            two = arrived[e * block_tiles + link[0, 1]].astype(F32)
            top = jnp.where(low, one, pltpu.roll(two, ranks, 1))
            bottom = jnp.where(low, pltpu.roll(one, ranks, 1), two)
            value = jnp.concatenate([top, bottom], axis=0)
            value = jnp.where(level < limits[t, pairs + e : pairs + e + 1], value, 0.0)
            picked[t, :, e * lanes : (e + 1) * lanes] = value.astype(BF)
    for t in range(rows):
        total = field[:, t * tile : (t + 1) * tile] + jnp.dot(
            picked[t], cu[t].reshape(parts * link_count * ranks, tile), preferred_element_type=F32
        )
        out[:, t * tile : (t + 1) * tile] = total.astype(out.dtype)


def residual(
    currents, shared_basis, self_v, self_u, self_rank, coupling_u, coupling_rank, link_tiles, incident
):
    row_count = lax.axis_size("row")
    dom_count = lax.axis_size("dom")
    col_count = lax.axis_size("col")
    _, angles, tile = currents.shape
    _, window_rows, tiles, ranks, _ = self_v.shape
    link_count = link_tiles.shape[-1]
    own = currents[0]
    lane = pl.pallas_call(
        lanes_kernel,
        out_shape=pltpu.VMEM((8, 2 * ranks), jnp.int32),
        out_specs=ONCHIP,
        cost_estimate=pl.CostEstimate(flops=1 << 34, bytes_accessed=1 << 25, transcendentals=0),
        compiler_params=LIMIT,
        name="lanes",
    )()
    own, lane = lax.optimization_barrier((own, lane))
    neighbour = swap(own, "row", 1)
    outgoing = pl.pallas_call(
        project_kernel,
        out_shape=pltpu.VMEM((dom_count * row_count, angles // 2, 2 * ranks), BF),
        in_specs=[ONCHIP, ONCHIP],
        out_specs=ONCHIP,
        compiler_params=LIMIT,
        name="project",
    )(*map(onchip, (currents[0], shared_basis[0])))
    arrived = exchange(outgoing, ("dom", "row"))
    near = jnp.stack([own, neighbour])
    far = {}
    for bits in (4, 6, 2):
        far[bits] = swap(near, "row", bits)
    limits = pl.pallas_call(
        limits_kernel,
        out_shape=pltpu.VMEM((window_rows, tiles // 2 + dom_count, 2 * ranks), jnp.int32),
        in_specs=[ONCHIP] * 3,
        out_specs=ONCHIP,
        compiler_params=LIMIT,
        name="limits",
    )(*map(onchip, (self_rank[0], coupling_rank[0], lane)))
    field = ()
    for kernel, currents_in in (
        (self_first_kernel, (near, far[4])), (self_second_kernel, (far[2], far[6]))
    ):
        onchip_in = (limits, *currents_in, *field)
        pair_block = (2, window_rows, 2, ranks, tile)
        field = (
            pl.pallas_call(
                kernel,
                out_shape=pltpu.VMEM((angles, window_rows * tile), F32),
                in_specs=[ONCHIP] * len(onchip_in) + [ANYWHERE] * 2,
                out_specs=ONCHIP,
                scratch_shapes=[
                    pltpu.VMEM(pair_block, BF),
                    pltpu.VMEM(pair_block, BF),
                    pltpu.SemaphoreType.DMA((4,)),
                ],
                compiler_params=LIMIT,
            )(*map(onchip, onchip_in), inhbm(self_v[0]), inhbm(self_u[0])),
        )
    partial = pl.pallas_call(
        coupled_kernel,
        out_shape=pltpu.VMEM((angles, window_rows * tile), BF),
        in_specs=[ONCHIP] * 5,
        out_specs=ONCHIP,
        scratch_shapes=[pltpu.VMEM((window_rows, angles, dom_count * link_count * ranks), BF)],
        compiler_params=LIMIT,
        name="coupled",
    )(*map(onchip, (link_tiles[0], limits, arrived, *field, coupling_u[0])))
    arrived = exchange(partial.reshape(col_count, angles // col_count, window_rows * tile), "col")
    return (incident[0] - arrived.astype(F32).sum(axis=0))[None]


def solution(mesh):
    return jax.shard_map(
        residual,
        mesh=mesh,
        in_specs=(
            P("dom", None, ("col", "row")),
            P("dom", None, "col"),
            P("dom", "row", "col", None, None),
            P("dom", "row", "col", None, None),
            P("dom", "row", "col"),
            P("dom", "row", None, "col", None, None),
            P("dom", "row", None, "col"),
            P("dom", "row", None, "col"),
            P("dom", "col", "row"),
        ),
        out_specs=P("dom", "col", "row"),
        check_vma=False,
    )
```
